512 devices in a mesh: seq: 64 (over z, y_hi, x), tp: 8 (over y_lo, core).
Axes of the slice: x: 4, y: 8 (y_hi: 2, y_lo: 4; y = y_hi * 4 + y_lo), z: 8, core: 2. Of those that a mesh axis runs over, the one named last changes fastest.
Arguments:
- tokens: bfloat16 [8192, 2048], P('seq', 'tp'), may hold values from -6 to 6
- ln_gain: bfloat16 [2048], replicated, may hold values from 0.5 to 4.1
- w_qkv: bfloat16 [3, 2048, 2048], P(None, None, 'tp'), may hold values from -0.15467961 to 0.15467961
- w_out: bfloat16 [2048, 2048], P('tp'), may hold values from -0.1875 to 0.1875
Outputs:
- mixed: bfloat16 [8192, 2048], P('seq', 'tp')
The draws below stay inside these ranges and needn't reach their ends.
All inputs are finite; a program needn't handle non-finite values.
Results may differ from the reference program's by a relative error of at most 0.011.
Values may be sent and summed in bfloat16 or wider, within the bound.
No kernel may reach another device: no remote copies, remote signals or barrier semaphores. Data moves between devices by JAX's collectives and lax.ppermute only.
A program may use at most 64 MiB of HBM per device.

```python
import jax
import jax.numpy as jnp
from jax import lax

D = 2048
HEADS = 16
HEAD_DIM = 128
SEQ = 8192


def draw_ln_gain(key, part):
    return jax.random.uniform(key, (D,), jnp.float32, 0.6, 1.4).astype(jnp.bfloat16)


def draw_tokens(key, part):
    normal_rows = jnp.clip(jax.random.normal(jax.random.fold_in(key, 11), (SEQ, D), jnp.float32), -6.0, 6.0)
    return normal_rows.astype(jnp.bfloat16)


def draw_w_qkv(key, part):
    bound_abs = 7.0 * D ** (-0.5)
    entries = jnp.clip(jax.random.normal(jax.random.fold_in(key, 23), (3, D, HEADS * HEAD_DIM), jnp.float32), -6.0, 6.0) * D ** (-0.5)
    return jnp.clip(entries, -bound_abs, bound_abs).astype(jnp.bfloat16)


def spiked(values, rng, source, target, parts, factor):
    def block_of(dim):
        return (jnp.arange(values.shape[dim]) // (values.shape[dim] // parts)).reshape((-1,) + (1,) * (values.ndim - 1 - dim))

    one_side = jax.random.permutation(rng, parts)[block_of(target)]
    other_side = (block_of(target) + parts // 2) % parts
    return jnp.where((block_of(source) == one_side) | (block_of(source) == other_side), factor * values, values)


def shard_levels(rng, shape, cuts, least, top_value):
    gain, own = 1.0, jax.random.fold_in(rng, 6)
    for axis_at, parts in cuts:
        draws = jnp.exp(jax.random.uniform(jax.random.fold_in(own, axis_at), (parts,), jnp.float32, least / len(cuts), top_value / len(cuts)))
        gain = gain * jnp.repeat(draws, shape[axis_at] // parts).reshape([-1 if axis == axis_at else 1 for axis in range(len(shape))])
    return gain


def gaussian_with(stream_key, shape, scale, most, split, heavy, kind=jnp.bfloat16):
    result = scale * jax.random.normal(stream_key, shape, jnp.float32)
    if split:
        result = result * shard_levels(stream_key, shape, split, -0.22, 0.18)
    return jnp.clip(spiked(result, jax.random.fold_in(stream_key, 3), *heavy), -most, most).astype(kind)


def setup_inputs(seed: int = 0) -> dict:
    seeds = jax.random.split(jax.random.key(seed), 5)
    return {
        "tokens": draw_tokens(jax.random.fold_in(seeds[4], 71), 0),
        "ln_gain": draw_ln_gain(jax.random.fold_in(seeds[4], 71), 0),
        "w_qkv": draw_w_qkv(jax.random.fold_in(seeds[4], 71), 0),
        "w_out": gaussian_with(seeds[3], (HEADS * HEAD_DIM, D), (HEADS * HEAD_DIM) ** -0.5, 0.1875, ((0, 8),), (0, 1, 8, 2.0)),
    }


def reference(tokens, ln_gain, w_qkv, w_out):
    values = tokens.astype(jnp.float32)
    average = lax.optimization_barrier(jnp.mean(values, axis=1, keepdims=True))
    second = lax.optimization_barrier(jnp.mean(values * values, axis=1, keepdims=True))
    normed = ((values - average) * lax.rsqrt(second - average * average + 1e-06) * ln_gain.astype(jnp.float32)).astype(jnp.bfloat16)
    queries = jnp.dot(normed, w_qkv[0], preferred_element_type=jnp.float32).astype(jnp.bfloat16).reshape(SEQ, HEADS, HEAD_DIM)
    keys_all = jnp.dot(normed, w_qkv[1], preferred_element_type=jnp.float32).astype(jnp.bfloat16).reshape(SEQ, HEADS, HEAD_DIM)
    vals_all = jnp.dot(normed, w_qkv[2], preferred_element_type=jnp.float32).astype(jnp.bfloat16).reshape(SEQ, HEADS, HEAD_DIM)
    span = min(512, SEQ)
    factor = HEAD_DIM ** (-0.5)
    keys_wide = keys_all.astype(jnp.float32)
    vals_wide = vals_all.astype(jnp.float32)

    def attend(offset):
        query_block = lax.dynamic_slice_in_dim(queries, offset, span, 0).astype(jnp.float32)
        scores = jnp.einsum('thc,shc->ths', query_block, keys_wide) * factor
        highest = lax.optimization_barrier(jnp.max(scores, axis=2, keepdims=True))
        expon = jnp.exp(scores - highest)
        denoms = lax.optimization_barrier(jnp.sum(expon, axis=2))
        weights = expon.astype(jnp.bfloat16).astype(jnp.float32)
        summed = jnp.einsum('ths,shc->thc', weights, vals_wide) / denoms[:, :, None]
        return summed.reshape(span, HEADS * HEAD_DIM).astype(jnp.bfloat16)
    offsets = jnp.arange(SEQ // span, dtype=jnp.int32) * span
    context = lax.map(attend, offsets).reshape(SEQ, HEADS * HEAD_DIM)
    projected = jnp.dot(context, w_out, preferred_element_type=jnp.float32)
    return (values + projected).astype(jnp.bfloat16)
```

```python
import functools
import math

import jax
import jax.numpy as jnp
from jax import lax
from jax.experimental import pallas as pl
from jax.experimental.pallas import tpu as pltpu
from jax.sharding import Mesh
from jax.sharding import PartitionSpec as P

HEAD_DIM = 128
ROWS = 128
GROUP = 8
STAT_ROWS = 8
LOG2E = math.log2(math.e)
bf16 = jnp.bfloat16
f32 = jnp.float32


def vmem(count):
    return [pl.BlockSpec(memory_space=pltpu.VMEM)] * count


def norm_project(x_ref, gain_ref, w_ref, q_ref, kv_ref):
    width = x_ref.shape[3]
    blocks = [(y, c) for y in range(4) for c in range(2)]
    total = jnp.zeros((ROWS, width), f32)
    squares = jnp.zeros((ROWS, width), f32)
    for y, c in blocks:
        part = x_ref[c, y].astype(f32)
        total += part
        squares += part * part
    features = width * len(blocks)
    average = jnp.sum(total, axis=1, keepdims=True) / features
    second = jnp.sum(squares, axis=1, keepdims=True) / features
    inverse = lax.rsqrt(second - average * average + 1e-6)
    sums = [jnp.zeros((ROWS, width), f32) for _ in range(3)]
    for t, (y, c) in enumerate(blocks):
        part = x_ref[c, y].astype(f32)
        gain = gain_ref[t : t + 1, :].astype(f32)
        normed = ((part - average) * inverse * gain).astype(bf16)
        for j in range(3):
            sums[j] += jnp.dot(
                normed, w_ref[j, t * width : (t + 1) * width, :], preferred_element_type=f32
            )
    query = sums[0].astype(bf16)
    key = sums[1].astype(bf16)
    value = sums[2]
    turned = jnp.concatenate(
        [value[:, h * HEAD_DIM : (h + 1) * HEAD_DIM].T for h in range(2)], axis=1
    ).astype(bf16)
    for i in range(GROUP):
        q_ref[i] = query
        kv_ref[i, :, : 2 * HEAD_DIM] = key
        kv_ref[i, :, 2 * HEAD_DIM :] = turned


def attend(q_ref, kv_ref, o_ref):
    factor = HEAD_DIM**-0.5 * LOG2E
    for h in range(2):
        cols = slice(h * HEAD_DIM, (h + 1) * HEAD_DIM)
        vcols = slice((2 + h) * HEAD_DIM, (3 + h) * HEAD_DIM)
        keys = kv_ref[:, :, cols].reshape(GROUP * ROWS, HEAD_DIM)
        values = jnp.concatenate([kv_ref[s, :, vcols] for s in range(GROUP)], axis=1)
        for pair in range(GROUP // 2):
            query = q_ref[2 * pair : 2 * pair + 2, :, cols].reshape(2 * ROWS, HEAD_DIM)
            scores = lax.dot_general(
                keys, query, (((1,), (1,)), ((), ())), preferred_element_type=f32
            )
            highest = jnp.max(scores, axis=0, keepdims=True)
            expon = jnp.exp2((scores - highest) * factor)
            denom = jnp.sum(expon, axis=0, keepdims=True)
            context = jnp.dot(values, expon.astype(bf16), preferred_element_type=f32)
            context = (context / denom).astype(bf16)
            level = highest * factor + jnp.log2(denom)
            first = level.astype(bf16).astype(f32)
            middle = (level - first).astype(bf16).astype(f32)
            last = level - first - middle
            stats = jnp.concatenate(
                [first, middle, last, jnp.zeros((STAT_ROWS - 3, 2 * ROWS), f32)], axis=0
            ).astype(bf16)
            for i in range(2):
                span = slice(i * ROWS, (i + 1) * ROWS)
                o_ref[2 * pair + i, :HEAD_DIM, cols] = context[:, span]
                o_ref[2 * pair + i, HEAD_DIM:, cols] = stats[:, span]


def combine(o_ref, c_ref):
    levels = []
    for s in range(GROUP):
        stats = o_ref[s, HEAD_DIM:, :].astype(f32)
        levels.append(stats[0:1] + stats[1:2] + stats[2:3])
    highest = functools.reduce(jnp.maximum, levels)
    shares = [jnp.exp2(level - highest) for level in levels]
    denom = functools.reduce(jnp.add, shares)
    total = jnp.zeros((HEAD_DIM, 2 * ROWS), f32)
    for s in range(GROUP):
        total += o_ref[s, :HEAD_DIM, :].astype(f32) * (shares[s] / denom)
    c_ref[...] = total.astype(bf16)


def project(own_ref, other_ref, w_ref, w_other_ref, out_ref):
    core = lax.axis_index("core")
    for y in range(4):
        cols = pl.ds(pl.multiple_of((2 * y + core) * 256, 256), 256)
        total = jnp.zeros((ROWS, 256), f32)
        for ctx, w in ((own_ref, w_ref), (other_ref, w_other_ref)):
            for h in range(2):
                total += lax.dot_general(
                    ctx[:, h * ROWS : (h + 1) * ROWS],
                    w[h * HEAD_DIM : (h + 1) * HEAD_DIM, cols],
                    (((0,), (0,)), ((), ())),
                    preferred_element_type=f32,
                )
        out_ref[y] = total.astype(bf16)


def spread(block, count):
    return jnp.broadcast_to(block[None], (count, *block.shape))


def exchange(blocks, axes):
    return lax.all_to_all(blocks, axes, 0, 0, tiled=True)


SWAP = ((0, 1), (1, 0))


def on_device(tokens, ln_gain, w_qkv, w_out):
    shape = jax.ShapeDtypeStruct
    across = exchange(spread(tokens, 4), "y_lo")
    w_other = lax.ppermute(w_out, "core", SWAP)
    whole = lax.all_gather(across, "core", axis=0)
    q_blocks, kv_blocks = pl.pallas_call(
        norm_project,
        out_shape=(shape((GROUP, ROWS, 256), bf16), shape((GROUP, ROWS, 512), bf16)),
        in_specs=vmem(3),
        out_specs=tuple(vmem(2)),
        cost_estimate=pl.CostEstimate(
            flops=2 * ROWS * 2048 * 768, bytes_accessed=5 << 20, transcendentals=0
        ),
    )(whole, ln_gain.reshape(8, 256), w_qkv)
    kv_here = exchange(kv_blocks, ("y_hi", "x"))
    q_here = exchange(q_blocks, "z")
    partial = pl.pallas_call(
        attend,
        out_shape=shape((GROUP, HEAD_DIM + STAT_ROWS, 2 * ROWS), bf16),
        in_specs=vmem(2),
        out_specs=vmem(1)[0],
        compiler_params=pltpu.CompilerParams(vmem_limit_bytes=40 << 20),
        cost_estimate=pl.CostEstimate(
            flops=4 * 1024 * 1024 * 256, bytes_accessed=3 << 20, transcendentals=2 << 20
        ),
    )(q_here, kv_here)
    shares = exchange(partial, "z")
    context = pl.pallas_call(
        combine,
        out_shape=shape((HEAD_DIM, 2 * ROWS), bf16),
        in_specs=vmem(1),
        out_specs=vmem(1)[0],
    )(shares)
    other = lax.ppermute(context, "core", SWAP)
    projected = pl.pallas_call(
        project,
        out_shape=shape((4, ROWS, 256), bf16),
        in_specs=vmem(4),
        out_specs=vmem(1)[0],
    )(context, other, w_out, w_other)
    summed = jnp.sum(exchange(projected, "y_lo").astype(f32), axis=0)
    return (tokens.astype(f32) + summed).astype(bf16)


def solution(mesh):
    grid = Mesh(mesh.devices.reshape(8, 2, 4, 4, 2), ("z", "y_hi", "x", "y_lo", "core"))
    seq, tp = ("z", "y_hi", "x"), ("y_lo", "core")
    return jax.shard_map(
        on_device,
        mesh=grid,
        in_specs=(P(seq, tp), P(), P(None, None, tp), P(tp, None)),
        out_specs=P(seq, tp),
        check_vma=False,
    )
```

```python
import functools
import math

import jax
import jax.numpy as jnp
from jax import lax
from jax.experimental import pallas as pl
from jax.experimental.pallas import tpu as pltpu
from jax.sharding import Mesh
from jax.sharding import PartitionSpec as P

HEAD_DIM = 128
ROWS = 128
GROUP = 8
STAT_ROWS = 8
LOG2E = math.log2(math.e)
bf16 = jnp.bfloat16
f32 = jnp.float32


def vmem(count):
    return [pl.BlockSpec(memory_space=pltpu.VMEM)] * count


def norm_project(x_ref, gain_ref, w_ref, q_ref, kv_ref):
    width = x_ref.shape[3]
    blocks = [(y, c) for y in range(4) for c in range(2)]
    total = jnp.zeros((ROWS, width), f32)
    squares = jnp.zeros((ROWS, width), f32)
    for y, c in blocks:
        part = x_ref[c, y].astype(f32)
        total += part
        squares += part * part
    features = width * len(blocks)
    average = jnp.sum(total, axis=1, keepdims=True) / features
    second = jnp.sum(squares, axis=1, keepdims=True) / features
    inverse = lax.rsqrt(second - average * average + 1e-6)
    sums = [jnp.zeros((ROWS, width), f32) for _ in range(3)]
    for t, (y, c) in enumerate(blocks):
        part = x_ref[c, y].astype(f32)
        gain = gain_ref[t : t + 1, :].astype(f32)
        normed = ((part - average) * inverse * gain).astype(bf16)
        for j in range(3):
            sums[j] += jnp.dot(
                normed, w_ref[j, t * width : (t + 1) * width, :], preferred_element_type=f32
            )
    query = sums[0].astype(bf16)
    key = sums[1].astype(bf16)
    value = sums[2]
    turned = jnp.concatenate(
        [value[:, h * HEAD_DIM : (h + 1) * HEAD_DIM].T for h in range(2)], axis=1
    ).astype(bf16)
    q_ref[...] = query
    for i in range(GROUP):
        kv_ref[i, :, : 2 * HEAD_DIM] = key
        kv_ref[i, :, 2 * HEAD_DIM :] = turned


def attend(q_ref, kv_ref, o_ref):
    factor = HEAD_DIM**-0.5 * LOG2E
    for h in range(2):
        cols = slice(h * HEAD_DIM, (h + 1) * HEAD_DIM)
        vcols = slice((2 + h) * HEAD_DIM, (3 + h) * HEAD_DIM)
        keys = kv_ref[:, :, cols].reshape(GROUP * ROWS, HEAD_DIM)
        values = jnp.concatenate([kv_ref[s, :, vcols] for s in range(GROUP)], axis=1)
        for pair in range(GROUP // 2):
            query = q_ref[2 * pair : 2 * pair + 2, :, cols].reshape(2 * ROWS, HEAD_DIM)
            scores = lax.dot_general(
                keys, query, (((1,), (1,)), ((), ())), preferred_element_type=f32
            )
            highest = jnp.max(scores, axis=0, keepdims=True)
            expon = jnp.exp2((scores - highest) * factor)
            denom = jnp.sum(expon, axis=0, keepdims=True)
            context = jnp.dot(values, expon.astype(bf16), preferred_element_type=f32)
            context = (context / denom).astype(bf16)
            level = highest * factor + jnp.log2(denom)
            first = level.astype(bf16).astype(f32)
            middle = (level - first).astype(bf16).astype(f32)
            last = level - first - middle
            stats = jnp.concatenate(
                [first, middle, last, jnp.zeros((STAT_ROWS - 3, 2 * ROWS), f32)], axis=0
            ).astype(bf16)
            for i in range(2):
                span = slice(i * ROWS, (i + 1) * ROWS)
                o_ref[2 * pair + i, :HEAD_DIM, cols] = context[:, span]
                o_ref[2 * pair + i, HEAD_DIM:, cols] = stats[:, span]


def combine(o_ref, c_ref):
    levels = []
    for s in range(GROUP):
        stats = o_ref[s, HEAD_DIM:, :].astype(f32)
        levels.append(stats[0:1] + stats[1:2] + stats[2:3])
    highest = functools.reduce(jnp.maximum, levels)
    shares = [jnp.exp2(level - highest) for level in levels]
    denom = functools.reduce(jnp.add, shares)
    total = jnp.zeros((HEAD_DIM, 2 * ROWS), f32)
    for s in range(GROUP):
        total += o_ref[s, :HEAD_DIM, :].astype(f32) * (shares[s] / denom)
    c_ref[...] = total.astype(bf16)


def project(ctx_ref, w_ref, w_other_ref, out_ref):
    core = lax.axis_index("core")
    turned = []
    for c in (core, 1 - core):
        context = ctx_ref[c]
        for h in range(2):
            turned.append(context[:, h * ROWS : (h + 1) * ROWS].T)
    turned = jnp.concatenate(turned, axis=1)
    for y in range(4):
        weights = jnp.concatenate([w_ref[:, y, :], w_other_ref[:, y, :]], axis=0)
        out_ref[y] = jnp.dot(turned, weights, preferred_element_type=f32).astype(bf16)


def spread(block, count):
    return jnp.broadcast_to(block[None], (count, *block.shape))


def exchange(blocks, axes):
    return lax.all_to_all(blocks, axes, 0, 0, tiled=True)


SWAP = ((0, 1), (1, 0))


def on_device(tokens, ln_gain, w_qkv, w_out):
    shape = jax.ShapeDtypeStruct
    across = exchange(spread(tokens, 4), "y_lo")
    w_cores = w_out.reshape(256, 4, 2, 256)
    core = lax.axis_index("core")
    w_own = lax.dynamic_index_in_dim(w_cores, core, 2, keepdims=False)
    w_other = lax.ppermute(
        lax.dynamic_index_in_dim(w_cores, 1 - core, 2, keepdims=False), "core", SWAP
    )
    whole = lax.all_gather(across, "core", axis=0)
    query, kv_blocks = pl.pallas_call(
        norm_project,
        out_shape=(shape((ROWS, 256), bf16), shape((GROUP, ROWS, 512), bf16)),
        in_specs=vmem(3),
        out_specs=tuple(vmem(2)),
        compiler_params=pltpu.CompilerParams(vmem_limit_bytes=24 << 20),
        cost_estimate=pl.CostEstimate(
            flops=2 * ROWS * 2048 * 768, bytes_accessed=5 << 20, transcendentals=0
        ),
    )(whole, ln_gain.reshape(8, 256), w_qkv)
    kv_here = exchange(kv_blocks, ("y_hi", "x"))
    q_here = lax.all_gather(query, "z", axis=0)
    partial = pl.pallas_call(
        attend,
        out_shape=shape((GROUP, HEAD_DIM + STAT_ROWS, 2 * ROWS), bf16),
        in_specs=vmem(2),
        out_specs=vmem(1)[0],
        compiler_params=pltpu.CompilerParams(vmem_limit_bytes=40 << 20),
        cost_estimate=pl.CostEstimate(
            flops=4 * 1024 * 1024 * 256, bytes_accessed=3 << 20, transcendentals=2 << 20
        ),
    )(q_here, kv_here)
    shares = exchange(partial, "z")
    context = pl.pallas_call(
        combine,
        out_shape=shape((HEAD_DIM, 2 * ROWS), bf16),
        in_specs=vmem(1),
        out_specs=vmem(1)[0],
        compiler_params=pltpu.CompilerParams(vmem_limit_bytes=16 << 20),
    )(shares)
    both = lax.all_gather(context, "core", axis=0)
    projected = pl.pallas_call(
        project,
        out_shape=shape((4, ROWS, 256), bf16),
        in_specs=vmem(3),
        out_specs=vmem(1)[0],
        compiler_params=pltpu.CompilerParams(vmem_limit_bytes=16 << 20),
    )(both, w_own, w_other)
    summed = jnp.sum(exchange(projected, "y_lo").astype(f32), axis=0)
    return (tokens.astype(f32) + summed).astype(bf16)


def solution(mesh):
    grid = Mesh(mesh.devices.reshape(8, 2, 4, 4, 2), ("z", "y_hi", "x", "y_lo", "core"))
    seq, tp = ("z", "y_hi", "x"), ("y_lo", "core")
    return jax.shard_map(
        on_device,
        mesh=grid,
        in_specs=(P(seq, tp), P(), P(None, None, tp), P(tp, None)),
        out_specs=P(seq, tp),
        check_vma=False,
    )
```

```python
import functools
import math

import jax
import jax.numpy as jnp
from jax import lax
from jax.experimental import pallas as pl
from jax.experimental.pallas import tpu as pltpu
from jax.sharding import Mesh
from jax.sharding import PartitionSpec as P

HEAD_DIM = 128
ROWS = 128
STAT_ROWS = 8
LOG2E = math.log2(math.e)
QUERY_GROUP = 8
KEY_GROUP = 4
SWAP = ((0, 1), (1, 0))
bf16 = jnp.bfloat16
f32 = jnp.float32
shape = jax.ShapeDtypeStruct


def vmem(count):
    return [pl.BlockSpec(memory_space=pltpu.VMEM)] * count


def limit(mib):
    return pltpu.CompilerParams(vmem_limit_bytes=mib << 20)


def repeat(tokens_ref, copies_ref):
    for i in range(4):
        copies_ref[i] = tokens_ref[...]


def norm_project(x_ref, gain_ref, w_ref, q_ref, kv_ref):
    width = x_ref.shape[3]
    gains = gain_ref[...].astype(f32).reshape(8, 256)
    blocks = [(y, c) for y in range(4) for c in range(2)]
    total = jnp.zeros((ROWS, width), f32)
    squares = jnp.zeros((ROWS, width), f32)
    for y, c in blocks:
        part = x_ref[c, y].astype(f32)
        total += part
        squares += part * part
    features = width * len(blocks)
    average = jnp.sum(total, axis=1, keepdims=True) / features
    second = jnp.sum(squares, axis=1, keepdims=True) / features
    inverse = lax.rsqrt(second - average * average + 1e-6)
    sums = [jnp.zeros((ROWS, width), f32) for _ in range(3)]
    for t, (y, c) in enumerate(blocks):
        part = x_ref[c, y].astype(f32)
        gain = gains[t : t + 1, :]
        normed = ((part - average) * inverse * gain).astype(bf16)
        for j in range(3):
            sums[j] += jnp.dot(
                normed, w_ref[j, t * width : (t + 1) * width, :], preferred_element_type=f32
            )
    query = sums[0].astype(bf16)
    q_ref[...] = query
    keys = sums[1].astype(bf16)
    turned = jnp.concatenate([sums[2][:, :HEAD_DIM].T, sums[2][:, HEAD_DIM:].T], axis=1).astype(bf16)
    for i in range(8):
        kv_ref[i, :, :256] = keys
        kv_ref[i, :, 256:] = turned


def attend(q_ref, kv_ref, o_ref):
    factor = HEAD_DIM**-0.5 * LOG2E
    for h in range(2):
        cols = slice(h * HEAD_DIM, (h + 1) * HEAD_DIM)
        vcols = slice((2 + h) * HEAD_DIM, (3 + h) * HEAD_DIM)
        keys = kv_ref[:, :, cols].reshape(2 * KEY_GROUP * ROWS, HEAD_DIM)
        values = jnp.concatenate(
            [
                kv_ref[s, a * ROWS : (a + 1) * ROWS, vcols]
                for s in range(KEY_GROUP)
                for a in range(2)
            ],
            axis=1,
        )
        for pair in range(QUERY_GROUP // 2):
            query = q_ref[2 * pair : 2 * pair + 2, :, cols].reshape(2 * ROWS, HEAD_DIM)
            scores = lax.dot_general(
                keys, query, (((1,), (1,)), ((), ())), preferred_element_type=f32
            )
            highest = jnp.max(scores, axis=0, keepdims=True)
            expon = jnp.exp2((scores - highest) * factor)
            denom = jnp.sum(expon, axis=0, keepdims=True)
            context = jnp.dot(values, expon.astype(bf16), preferred_element_type=f32)
            context = (context / denom).astype(bf16)
            level = highest * factor + jnp.log2(denom)
            first = level.astype(bf16).astype(f32)
            middle = (level - first).astype(bf16).astype(f32)
            last = level - first - middle
            stats = jnp.concatenate(
                [first, middle, last, jnp.zeros((STAT_ROWS - 3, 2 * ROWS), f32)], axis=0
            ).astype(bf16)
            for i in range(2):
                span = slice(i * ROWS, (i + 1) * ROWS)
                o_ref[2 * pair + i, :HEAD_DIM, cols] = context[:, span]
                o_ref[2 * pair + i, HEAD_DIM:, cols] = stats[:, span]


def combine(o_ref, c_ref):
    levels = []
    for s in range(QUERY_GROUP):
        stats = o_ref[s, HEAD_DIM:, :].astype(f32)
        levels.append(stats[0:1] + stats[1:2] + stats[2:3])
    highest = functools.reduce(jnp.maximum, levels)
    shares = [jnp.exp2(level - highest) for level in levels]
    denom = functools.reduce(jnp.add, shares)
    total = jnp.zeros((HEAD_DIM, 2 * ROWS), f32)
    for s in range(QUERY_GROUP):
        total += o_ref[s, :HEAD_DIM, :].astype(f32) * (shares[s] / denom)
    c_ref[...] = total.astype(bf16)


def project(ctx_ref, w_ref, w_other_ref, out_ref):
    core = lax.axis_index("core")
    turned = []
    for c in (core, 1 - core):
        context = ctx_ref[c]
        for h in range(2):
            turned.append(context[:, h * ROWS : (h + 1) * ROWS].T)
    turned = jnp.concatenate(turned, axis=1)
    for y in range(4):
        cols = pl.ds(pl.multiple_of((2 * y + core) * 256, 256), 256)
        weights = jnp.concatenate([w_ref[:, cols], w_other_ref[:, cols]], axis=0)
        out_ref[y] = jnp.dot(turned, weights, preferred_element_type=f32).astype(bf16)


def exchange(blocks, axes):
    return lax.all_to_all(blocks, axes, 0, 0, tiled=True)


def on_device(tokens, ln_gain, w_qkv, w_out):
    copies = pl.pallas_call(
        repeat,
        out_shape=shape((4, *tokens.shape), bf16),
        in_specs=vmem(1),
        out_specs=vmem(1)[0],
        compiler_params=limit(4),
    )(tokens)
    across = exchange(copies, "y_lo")
    w_other = lax.ppermute(w_out, "core", SWAP)
    whole = lax.all_gather(across, "core", axis=0)
    q_blocks, kv_near = pl.pallas_call(
        norm_project,
        out_shape=(shape((ROWS, 256), bf16), shape((8, ROWS, 512), bf16)),
        in_specs=vmem(3),
        out_specs=tuple(vmem(2)),
        compiler_params=limit(24),
        cost_estimate=pl.CostEstimate(
            flops=2 * ROWS * 2048 * 768, bytes_accessed=5 << 20, transcendentals=0
        ),
    )(whole, ln_gain, w_qkv)
    kv_here = exchange(kv_near, ("y_hi", "x")).reshape(4, 256, 512)
    q_here = lax.all_gather(q_blocks, "z", axis=0)
    partial = pl.pallas_call(
        attend,
        out_shape=shape((QUERY_GROUP, HEAD_DIM + STAT_ROWS, 2 * ROWS), bf16),
        in_specs=vmem(2),
        out_specs=vmem(1)[0],
        compiler_params=limit(24),
        cost_estimate=pl.CostEstimate(
            flops=4 * 1024 * 1024 * 256, bytes_accessed=3 << 20, transcendentals=2 << 20
        ),
    )(q_here, kv_here)
    shares = exchange(partial, "z")
    context = pl.pallas_call(
        combine,
        out_shape=shape((HEAD_DIM, 2 * ROWS), bf16),
        in_specs=vmem(1),
        out_specs=vmem(1)[0],
        compiler_params=limit(16),
    )(shares)
    projected = pl.pallas_call(
        project,
        out_shape=shape((4, ROWS, 256), bf16),
        in_specs=vmem(3),
        out_specs=vmem(1)[0],
        compiler_params=limit(16),
    )(lax.all_gather(context, "core", axis=0), w_out, w_other)
    summed = jnp.sum(exchange(projected, "y_lo").astype(f32), axis=0)
    return (tokens.astype(f32) + summed).astype(bf16)


def solution(mesh):
    grid = Mesh(mesh.devices.reshape(8, 2, 4, 4, 2), ("z", "y_hi", "x", "y_lo", "core"))
    seq, tp = ("z", "y_hi", "x"), ("y_lo", "core")
    return jax.shard_map(
        on_device,
        mesh=grid,
        in_specs=(P(seq, tp), P(), P(None, None, tp), P(tp, None)),
        out_specs=P(seq, tp),
        check_vma=False,
    )
```

```python
import functools
import math

import jax
import jax.numpy as jnp
from jax import lax
from jax.experimental import pallas as pl
from jax.experimental.pallas import tpu as pltpu
from jax.sharding import Mesh
from jax.sharding import PartitionSpec as P

HEAD_DIM = 128
ROWS = 128
STAT_ROWS = 8
LOG2E = math.log2(math.e)
QUERY_GROUP = 8
KEY_GROUP = 4
SWAP = ((0, 1), (1, 0))
bf16 = jnp.bfloat16
f32 = jnp.float32
shape = jax.ShapeDtypeStruct


def vmem(count):
    return [pl.BlockSpec(memory_space=pltpu.VMEM)] * count


def limit(mib):
    return pltpu.CompilerParams(vmem_limit_bytes=mib << 20)


def repeat(tokens_ref, copies_ref):
    for i in range(4):
        copies_ref[i] = tokens_ref[...]


def norm_project(x_ref, gain_ref, wq_ref, wk_ref, wv_ref, q_ref, kv_ref):
    w_refs = (wq_ref, wk_ref, wv_ref)
    width = x_ref.shape[3]
    gains = gain_ref[...].astype(f32).reshape(8, 256)
    blocks = [(y, c) for y in range(4) for c in range(2)]
    total = jnp.zeros((ROWS, width), f32)
    squares = jnp.zeros((ROWS, width), f32)
    for y, c in blocks:
        part = x_ref[c, y].astype(f32)
        total += part
        squares += part * part
    features = width * len(blocks)
    average = jnp.sum(total, axis=1, keepdims=True) / features
    second = jnp.sum(squares, axis=1, keepdims=True) / features
    inverse = lax.rsqrt(second - average * average + 1e-6)
    sums = [jnp.zeros((ROWS, width), f32) for _ in range(3)]
    for t, (y, c) in enumerate(blocks):
        part = x_ref[c, y].astype(f32)
        gain = gains[t : t + 1, :]
        normed = ((part - average) * inverse * gain).astype(bf16)
        for j in range(3):
            sums[j] += jnp.dot(
                normed, w_refs[j][t * width : (t + 1) * width, :], preferred_element_type=f32
            )
    query = sums[0].astype(bf16)
    q_ref[...] = query
    keys = sums[1].astype(bf16)
    turned = jnp.concatenate([sums[2][:, :HEAD_DIM].T, sums[2][:, HEAD_DIM:].T], axis=1).astype(bf16)
    for i in range(8):
        kv_ref[i, :, :256] = keys
        kv_ref[i, :, 256:] = turned


def attend(q_ref, kv_ref, o_ref):
    factor = HEAD_DIM**-0.5 * LOG2E
    for h in range(2):
        cols = slice(h * HEAD_DIM, (h + 1) * HEAD_DIM)
        vcols = slice((2 + h) * HEAD_DIM, (3 + h) * HEAD_DIM)
        keys = kv_ref[:, :, cols].reshape(2 * KEY_GROUP * ROWS, HEAD_DIM)
        values = jnp.concatenate(
            [
                kv_ref[s, a * ROWS : (a + 1) * ROWS, vcols]
                for s in range(KEY_GROUP)
                for a in range(2)
            ],
            axis=1,
        )
        for pair in range(QUERY_GROUP // 2):
            query = q_ref[2 * pair : 2 * pair + 2, :, cols].reshape(2 * ROWS, HEAD_DIM)
            scores = lax.dot_general(
                keys, query, (((1,), (1,)), ((), ())), preferred_element_type=f32
            )
            highest = jnp.max(scores, axis=0, keepdims=True)
            expon = jnp.exp2((scores - highest) * factor)
            denom = jnp.sum(expon, axis=0, keepdims=True)
            context = jnp.dot(values, expon.astype(bf16), preferred_element_type=f32)
            context = (context / denom).astype(bf16)
            level = highest * factor + jnp.log2(denom)
            first = level.astype(bf16).astype(f32)
            middle = (level - first).astype(bf16).astype(f32)
            last = level - first - middle
            stats = jnp.concatenate(
                [first, middle, last, jnp.zeros((STAT_ROWS - 3, 2 * ROWS), f32)], axis=0
            ).astype(bf16)
            for i in range(2):
                span = slice(i * ROWS, (i + 1) * ROWS)
                o_ref[2 * pair + i, :HEAD_DIM, cols] = context[:, span]
                o_ref[2 * pair + i, HEAD_DIM:, cols] = stats[:, span]


def combine(o_ref, c_ref):
    levels = []
    for s in range(QUERY_GROUP):
        stats = o_ref[s, HEAD_DIM:, :].astype(f32)
        levels.append(stats[0:1] + stats[1:2] + stats[2:3])
    highest = functools.reduce(jnp.maximum, levels)
    shares = [jnp.exp2(level - highest) for level in levels]
    denom = functools.reduce(jnp.add, shares)
    total = jnp.zeros((HEAD_DIM, 2 * ROWS), f32)
    for s in range(QUERY_GROUP):
        total += o_ref[s, :HEAD_DIM, :].astype(f32) * (shares[s] / denom)
    c_ref[...] = total.astype(bf16)


def project(ctx_ref, w_ref, w_other_ref, out_ref):
    core = lax.axis_index("core")
    turned = []
    for c in (core, 1 - core):
        context = ctx_ref[c]
        for h in range(2):
            turned.append(context[:, h * ROWS : (h + 1) * ROWS].T)
    turned = jnp.concatenate(turned, axis=1)
    for y in range(4):
        cols = pl.ds(pl.multiple_of((2 * y + core) * 256, 256), 256)
        weights = jnp.concatenate([w_ref[:, cols], w_other_ref[:, cols]], axis=0)
        out_ref[y] = jnp.dot(turned, weights, preferred_element_type=f32).astype(bf16)


def exchange(blocks, axes):
    return lax.all_to_all(blocks, axes, 0, 0, tiled=True)


def on_device(tokens, ln_gain, w_qkv, w_out):
    copies = pl.pallas_call(
        repeat,
        out_shape=shape((4, *tokens.shape), bf16),
        in_specs=vmem(1),
        out_specs=vmem(1)[0],
        compiler_params=limit(4),
    )(tokens)
    across = exchange(copies, "y_lo")
    w_other = lax.ppermute(w_out, "core", SWAP)
    whole = lax.all_gather(across, "core", axis=0)
    q_blocks, kv_near = pl.pallas_call(
        norm_project,
        out_shape=(shape((ROWS, 256), bf16), shape((8, ROWS, 512), bf16)),
        in_specs=vmem(5),
        out_specs=tuple(vmem(2)),
        compiler_params=limit(24),
        cost_estimate=pl.CostEstimate(
            flops=2 * ROWS * 2048 * 768, bytes_accessed=5 << 20, transcendentals=0
        ),
    )(whole, ln_gain, w_qkv[0], w_qkv[1], w_qkv[2])
    kv_here = exchange(kv_near, ("y_hi", "x")).reshape(4, 256, 512)
    q_here = lax.all_gather(q_blocks, "z", axis=0)
    partial = pl.pallas_call(
        attend,
        out_shape=shape((QUERY_GROUP, HEAD_DIM + STAT_ROWS, 2 * ROWS), bf16),
        in_specs=vmem(2),
        out_specs=vmem(1)[0],
        compiler_params=limit(24),
        cost_estimate=pl.CostEstimate(
            flops=4 * 1024 * 1024 * 256, bytes_accessed=3 << 20, transcendentals=2 << 20
        ),
    )(q_here, kv_here)
    shares = exchange(partial, "z")
    context = pl.pallas_call(
        combine,
        out_shape=shape((HEAD_DIM, 2 * ROWS), bf16),
        in_specs=vmem(1),
        out_specs=vmem(1)[0],
        compiler_params=limit(16),
    )(shares)
    projected = pl.pallas_call(
        project,
        out_shape=shape((4, ROWS, 256), bf16),
        in_specs=vmem(3),
        out_specs=vmem(1)[0],
        compiler_params=limit(16),
    )(lax.all_gather(context, "core", axis=0), w_out, w_other)
    summed = jnp.sum(exchange(projected, "y_lo").astype(f32), axis=0)
    return (tokens.astype(f32) + summed).astype(bf16)


def solution(mesh):
    grid = Mesh(mesh.devices.reshape(8, 2, 4, 4, 2), ("z", "y_hi", "x", "y_lo", "core"))
    seq, tp = ("z", "y_hi", "x"), ("y_lo", "core")
    return jax.shard_map(
        on_device,
        mesh=grid,
        in_specs=(P(seq, tp), P(), P(None, None, tp), P(tp, None)),
        out_specs=P(seq, tp),
        check_vma=False,
    )
```

```python
import functools
import math

import jax
import jax.numpy as jnp
from jax import lax
from jax.experimental import pallas as pl
from jax.experimental.pallas import tpu as pltpu
from jax.sharding import Mesh
from jax.sharding import PartitionSpec as P

HEAD_DIM = 128
ROWS = 128
STAT_ROWS = 8
LOG2E = math.log2(math.e)
QUERY_GROUP = 8
KEY_GROUP = 4
SWAP = ((0, 1), (1, 0))
bf16 = jnp.bfloat16
f32 = jnp.float32
shape = jax.ShapeDtypeStruct


def vmem(count):
    return [pl.BlockSpec(memory_space=pltpu.VMEM)] * count


def limit(mib):
    return pltpu.CompilerParams(vmem_limit_bytes=mib << 20)


def repeat(tokens_ref, copies_ref):
    for i in range(4):
        copies_ref[i] = tokens_ref[...]


def norm_project(x_ref, gain_ref, wq_ref, wk_ref, wv_ref, q_ref, kv_ref):
    w_refs = (wq_ref, wk_ref, wv_ref)
    width = x_ref.shape[3]
    gains = gain_ref[...].astype(f32).reshape(8, 256)
    blocks = [(y, c) for y in range(4) for c in range(2)]
    total = jnp.zeros((ROWS, width), f32)
    squares = jnp.zeros((ROWS, width), f32)
    for y, c in blocks:
        part = x_ref[c, y].astype(f32)
        total += part
        squares += part * part
    features = width * len(blocks)
    average = jnp.sum(total, axis=1, keepdims=True) / features
    second = jnp.sum(squares, axis=1, keepdims=True) / features
    inverse = lax.rsqrt(second - average * average + 1e-6)
    sums = [jnp.zeros((ROWS, width), f32) for _ in range(3)]
    for t, (y, c) in enumerate(blocks):
        part = x_ref[c, y].astype(f32)
        gain = gains[t : t + 1, :]
        normed = ((part - average) * inverse * gain).astype(bf16)
        for j in range(3):
            sums[j] += jnp.dot(
                normed, w_refs[j][t * width : (t + 1) * width, :], preferred_element_type=f32
            )
    query = sums[0].astype(bf16)
    q_ref[...] = query
    keys = sums[1].astype(bf16)
    turned = jnp.concatenate([sums[2][:, :HEAD_DIM].T, sums[2][:, HEAD_DIM:].T], axis=1).astype(bf16)
    for i in range(8):
        kv_ref[i, :, :256] = keys
        kv_ref[i, :, 256:] = turned


def attend(q_ref, kv_ref, o_ref, parts, sent):
    factor = HEAD_DIM**-0.5 * LOG2E
    copies = []
    keys, values = [], []
    for h in range(2):
        cols = slice(h * HEAD_DIM, (h + 1) * HEAD_DIM)
        vcols = slice((2 + h) * HEAD_DIM, (3 + h) * HEAD_DIM)
        keys.append(kv_ref[:, :, cols].reshape(2 * KEY_GROUP * ROWS, HEAD_DIM))
        values.append(
            jnp.concatenate(
                [
                    kv_ref[s, a * ROWS : (a + 1) * ROWS, vcols]
                    for s in range(KEY_GROUP)
                    for a in range(2)
                ],
                axis=1,
            )
        )
    for pair in range(QUERY_GROUP // 2):
        for h in range(2):
            cols = slice(h * HEAD_DIM, (h + 1) * HEAD_DIM)
            query = q_ref[2 * pair : 2 * pair + 2, :, cols].reshape(2 * ROWS, HEAD_DIM)
            scores = lax.dot_general(
                keys[h], query, (((1,), (1,)), ((), ())), preferred_element_type=f32
            )
            highest = jnp.max(scores, axis=0, keepdims=True)
            expon = jnp.exp2((scores - highest) * factor)
            denom = jnp.sum(expon, axis=0, keepdims=True)
            context = jnp.dot(values[h], expon.astype(bf16), preferred_element_type=f32)
            context = (context / denom).astype(bf16)
            level = highest * factor + jnp.log2(denom)
            first = level.astype(bf16).astype(f32)
            middle = (level - first).astype(bf16).astype(f32)
            last = level - first - middle
            stats = jnp.concatenate(
                [first, middle, last, jnp.zeros((STAT_ROWS - 3, 2 * ROWS), f32)], axis=0
            ).astype(bf16)
            for i in range(2):
                span = slice(i * ROWS, (i + 1) * ROWS)
                parts[2 * pair + i, :HEAD_DIM, cols] = context[:, span]
                parts[2 * pair + i, HEAD_DIM:, cols] = stats[:, span]
        blocks = pl.ds(2 * pair, 2)
        copies.append(pltpu.make_async_copy(parts.at[blocks], o_ref.at[blocks], sent.at[pair]))
        copies[-1].start()
    for copy in copies:
        copy.wait()


def combine(o_ref, c_ref):
    levels = []
    for s in range(QUERY_GROUP):
        stats = o_ref[s, HEAD_DIM:, :].astype(f32)
        levels.append(stats[0:1] + stats[1:2] + stats[2:3])
    highest = functools.reduce(jnp.maximum, levels)
    shares = [jnp.exp2(level - highest) for level in levels]
    denom = functools.reduce(jnp.add, shares)
    total = jnp.zeros((HEAD_DIM, 2 * ROWS), f32)
    for s in range(QUERY_GROUP):
        total += o_ref[s, :HEAD_DIM, :].astype(f32) * (shares[s] / denom)
    c_ref[...] = total.astype(bf16)


def project(ctx_ref, w_ref, w_other_ref, out_ref):
    core = lax.axis_index("core")
    turned = []
    for c in (core, 1 - core):
        context = ctx_ref[c]
        for h in range(2):
            turned.append(context[:, h * ROWS : (h + 1) * ROWS].T)
    turned = jnp.concatenate(turned, axis=1)
    for y in range(4):
        cols = pl.ds(pl.multiple_of((2 * y + core) * 256, 256), 256)
        weights = jnp.concatenate([w_ref[:, cols], w_other_ref[:, cols]], axis=0)
        out_ref[y] = jnp.dot(turned, weights, preferred_element_type=f32).astype(bf16)


def exchange(blocks, axes):
    return lax.all_to_all(blocks, axes, 0, 0, tiled=True)


def on_device(tokens, ln_gain, w_qkv, w_out):
    copies = pl.pallas_call(
        repeat,
        out_shape=shape((4, *tokens.shape), bf16),
        in_specs=vmem(1),
        out_specs=vmem(1)[0],
        compiler_params=limit(4),
    )(tokens)
    across = exchange(copies, "y_lo")
    w_other = lax.ppermute(w_out, "core", SWAP)
    whole = lax.all_gather(across, "core", axis=0)
    q_blocks, kv_near = pl.pallas_call(
        norm_project,
        out_shape=(shape((ROWS, 256), bf16), shape((8, ROWS, 512), bf16)),
        in_specs=vmem(5),
        out_specs=tuple(vmem(2)),
        compiler_params=limit(24),
        cost_estimate=pl.CostEstimate(
            flops=2 * ROWS * 2048 * 768, bytes_accessed=5 << 20, transcendentals=0
        ),
    )(whole, ln_gain, w_qkv[0], w_qkv[1], w_qkv[2])
    kv_here = exchange(kv_near, ("y_hi", "x")).reshape(4, 256, 512)
    q_here = lax.all_gather(q_blocks, "z", axis=0)
    partial = pl.pallas_call(
        attend,
        out_shape=shape((QUERY_GROUP, HEAD_DIM + STAT_ROWS, 2 * ROWS), bf16),
        in_specs=vmem(2),
        out_specs=pl.BlockSpec(memory_space=pl.ANY),
        scratch_shapes=[
            pltpu.VMEM((QUERY_GROUP, HEAD_DIM + STAT_ROWS, 2 * ROWS), bf16),
            pltpu.SemaphoreType.DMA((QUERY_GROUP // 2,)),
        ],
        compiler_params=limit(24),
        cost_estimate=pl.CostEstimate(
            flops=4 * 1024 * 1024 * 256, bytes_accessed=3 << 20, transcendentals=2 << 20
        ),
    )(q_here, kv_here)
    shares = exchange(partial, "z")
    context = pl.pallas_call(
        combine,
        out_shape=shape((HEAD_DIM, 2 * ROWS), bf16),
        in_specs=vmem(1),
        out_specs=vmem(1)[0],
        compiler_params=limit(16),
    )(shares)
    projected = pl.pallas_call(
        project,
        out_shape=shape((4, ROWS, 256), bf16),
        in_specs=vmem(3),
        out_specs=vmem(1)[0],
        compiler_params=limit(16),
    )(lax.all_gather(context, "core", axis=0), w_out, w_other)
    summed = jnp.sum(exchange(projected, "y_lo").astype(f32), axis=0)
    return (tokens.astype(f32) + summed).astype(bf16)


def solution(mesh):
    grid = Mesh(mesh.devices.reshape(8, 2, 4, 4, 2), ("z", "y_hi", "x", "y_lo", "core"))
    seq, tp = ("z", "y_hi", "x"), ("y_lo", "core")
    return jax.shard_map(
        on_device,
        mesh=grid,
        in_specs=(P(seq, tp), P(), P(None, None, tp), P(tp, None)),
        out_specs=P(seq, tp),
        check_vma=False,
    )
```

```python
import functools
import math

import jax
import jax.numpy as jnp
from jax import lax
from jax.experimental import pallas as pl
from jax.experimental.pallas import tpu as pltpu
from jax.sharding import Mesh
from jax.sharding import PartitionSpec as P

HEAD_DIM = 128
ROWS = 128
STAT_ROWS = 8
LOG2E = math.log2(math.e)
QUERY_GROUP = 8
KEY_GROUP = 4
SWAP = ((0, 1), (1, 0))
bf16 = jnp.bfloat16
f32 = jnp.float32
shape = jax.ShapeDtypeStruct


def vmem(count):
    return [pl.BlockSpec(memory_space=pltpu.VMEM)] * count


def limit(mib):
    return pltpu.CompilerParams(vmem_limit_bytes=mib << 20)


def repeat(tokens_ref, copies_ref):
    for i in range(4):
        copies_ref[i] = tokens_ref[...]


def norm_project(x_ref, gain_ref, wq_ref, wk_ref, wv_ref, q_ref, kv_ref):
    w_refs = (wq_ref, wk_ref, wv_ref)
    width = x_ref.shape[3]
    gains = gain_ref[...].astype(f32).reshape(8, 256)
    blocks = [(y, c) for y in range(4) for c in range(2)]
    total = jnp.zeros((ROWS, width), f32)
    squares = jnp.zeros((ROWS, width), f32)
    for y, c in blocks:
        part = x_ref[c, y].astype(f32)
        total += part
        squares += part * part
    features = width * len(blocks)
    average = jnp.sum(total, axis=1, keepdims=True) / features
    second = jnp.sum(squares, axis=1, keepdims=True) / features
    inverse = lax.rsqrt(second - average * average + 1e-6)
    sums = [jnp.zeros((ROWS, width), f32) for _ in range(3)]
    for t, (y, c) in enumerate(blocks):
        part = x_ref[c, y].astype(f32)
        gain = gains[t : t + 1, :]
        normed = ((part - average) * inverse * gain).astype(bf16)
        for j in range(3):
            sums[j] += jnp.dot(
                normed, w_refs[j][t * width : (t + 1) * width, :], preferred_element_type=f32
            )
    query = sums[0].astype(bf16)
    q_ref[...] = query
    keys = sums[1].astype(bf16)
    turned = jnp.concatenate([sums[2][:, :HEAD_DIM].T, sums[2][:, HEAD_DIM:].T], axis=1).astype(bf16)
    for i in range(8):
        kv_ref[i, :, :256] = keys
        kv_ref[i, :, 256:] = turned


def attend(q_ref, kv_ref, o_ref, parts, sent):
    factor = HEAD_DIM**-0.5 * LOG2E
    copies = []
    keys, values = [], []
    for h in range(2):
        cols = slice(h * HEAD_DIM, (h + 1) * HEAD_DIM)
        vcols = slice((2 + h) * HEAD_DIM, (3 + h) * HEAD_DIM)
        keys.append(kv_ref[:, :, cols].reshape(2 * KEY_GROUP * ROWS, HEAD_DIM))
        values.append(
            jnp.concatenate(
                [
                    kv_ref[s, a * ROWS : (a + 1) * ROWS, vcols]
                    for s in range(KEY_GROUP)
                    for a in range(2)
                ],
                axis=1,
            )
        )
    for pair in range(QUERY_GROUP // 2):
        for h in range(2):
            cols = slice(h * HEAD_DIM, (h + 1) * HEAD_DIM)
            query = q_ref[2 * pair : 2 * pair + 2, :, cols].reshape(2 * ROWS, HEAD_DIM)
            scores = lax.dot_general(
                keys[h], query, (((1,), (1,)), ((), ())), preferred_element_type=f32
            )
            highest = jnp.max(scores, axis=0, keepdims=True)
            expon = jnp.exp2((scores - highest) * factor)
            denom = jnp.sum(expon, axis=0, keepdims=True)
            context = jnp.dot(values[h], expon.astype(bf16), preferred_element_type=f32)
            context = (context / denom).astype(bf16)
            level = highest * factor + jnp.log2(denom)
            first = level.astype(bf16).astype(f32)
            middle = (level - first).astype(bf16).astype(f32)
            last = level - first - middle
            stats = jnp.concatenate(
                [first, middle, last, jnp.zeros((STAT_ROWS - 3, 2 * ROWS), f32)], axis=0
            ).astype(bf16)
            for i in range(2):
                span = slice(i * ROWS, (i + 1) * ROWS)
                parts[2 * pair + i, :HEAD_DIM, cols] = context[:, span]
                parts[2 * pair + i, HEAD_DIM:, cols] = stats[:, span]
        blocks = pl.ds(2 * pair, 2)
        copies.append(pltpu.make_async_copy(parts.at[blocks], o_ref.at[blocks], sent.at[pair]))
        copies[-1].start()
    for copy in copies:
        copy.wait()


def combine(o_ref, c_ref):
    levels = []
    for s in range(QUERY_GROUP):
        stats = o_ref[s, HEAD_DIM:, :].astype(f32)
        levels.append(stats[0:1] + stats[1:2] + stats[2:3])
    highest = functools.reduce(jnp.maximum, levels)
    shares = [jnp.exp2(level - highest) for level in levels]
    denom = functools.reduce(jnp.add, shares)
    total = jnp.zeros((HEAD_DIM, 2 * ROWS), f32)
    for s in range(QUERY_GROUP):
        total += o_ref[s, :HEAD_DIM, :].astype(f32) * (shares[s] / denom)
    c_ref[...] = total.astype(bf16)


def project(ctx_ref, w_ref, w_other_ref, out_ref):
    core = lax.axis_index("core")
    turned = []
    for c in (core, 1 - core):
        context = ctx_ref[c]
        for h in range(2):
            turned.append(context[:, h * ROWS : (h + 1) * ROWS].T)
    turned = jnp.concatenate(turned, axis=1)
    for y in range(4):
        cols = pl.ds(pl.multiple_of((2 * y + core) * 256, 256), 256)
        weights = jnp.concatenate([w_ref[:, cols], w_other_ref[:, cols]], axis=0)
        out_ref[y] = jnp.dot(turned, weights, preferred_element_type=f32).astype(bf16)


def finish(tokens_ref, parts_ref, out_ref):
    total = parts_ref[0].astype(f32)
    for y in range(1, 4):
        total += parts_ref[y].astype(f32)
    out_ref[...] = (tokens_ref[...].astype(f32) + total).astype(bf16)


def exchange(blocks, axes):
    return lax.all_to_all(blocks, axes, 0, 0, tiled=True)


def on_device(tokens, ln_gain, w_qkv, w_out):
    copies = pl.pallas_call(
        repeat,
        out_shape=shape((4, *tokens.shape), bf16),
        in_specs=vmem(1),
        out_specs=vmem(1)[0],
        compiler_params=limit(4),
    )(tokens)
    across = exchange(copies, "y_lo")
    w_other = lax.ppermute(w_out, "core", SWAP)
    whole = lax.all_gather(across, "core", axis=0)
    q_blocks, kv_near = pl.pallas_call(
        norm_project,
        out_shape=(shape((ROWS, 256), bf16), shape((8, ROWS, 512), bf16)),
        in_specs=vmem(5),
        out_specs=tuple(vmem(2)),
        compiler_params=limit(24),
        cost_estimate=pl.CostEstimate(
            flops=2 * ROWS * 2048 * 768, bytes_accessed=5 << 20, transcendentals=0
        ),
    )(whole, ln_gain, w_qkv[0], w_qkv[1], w_qkv[2])
    kv_here = exchange(kv_near, ("y_hi", "x")).reshape(4, 256, 512)
    q_here = lax.all_gather(q_blocks, "z", axis=0)
    partial = pl.pallas_call(
        attend,
        out_shape=shape((QUERY_GROUP, HEAD_DIM + STAT_ROWS, 2 * ROWS), bf16),
        in_specs=vmem(2),
        out_specs=pl.BlockSpec(memory_space=pl.ANY),
        scratch_shapes=[
            pltpu.VMEM((QUERY_GROUP, HEAD_DIM + STAT_ROWS, 2 * ROWS), bf16),
            pltpu.SemaphoreType.DMA((QUERY_GROUP // 2,)),
        ],
        compiler_params=limit(24),
        cost_estimate=pl.CostEstimate(
            flops=4 * 1024 * 1024 * 256, bytes_accessed=3 << 20, transcendentals=2 << 20
        ),
    )(q_here, kv_here)
    shares = exchange(partial, "z")
    context = pl.pallas_call(
        combine,
        out_shape=shape((HEAD_DIM, 2 * ROWS), bf16),
        in_specs=vmem(1),
        out_specs=vmem(1)[0],
        compiler_params=limit(16),
    )(shares)
    projected = pl.pallas_call(
        project,
        out_shape=shape((4, ROWS, 256), bf16),
        in_specs=vmem(3),
        out_specs=vmem(1)[0],
        compiler_params=limit(16),
    )(lax.all_gather(context, "core", axis=0), w_out, w_other)
    return pl.pallas_call(
        finish,
        out_shape=shape(tokens.shape, bf16),
        in_specs=vmem(2),
        out_specs=vmem(1)[0],
        compiler_params=limit(4),
    )(tokens, exchange(projected, "y_lo"))


def solution(mesh):
    grid = Mesh(mesh.devices.reshape(8, 2, 4, 4, 2), ("z", "y_hi", "x", "y_lo", "core"))
    seq, tp = ("z", "y_hi", "x"), ("y_lo", "core")
    return jax.shard_map(
        on_device,
        mesh=grid,
        in_specs=(P(seq, tp), P(), P(None, None, tp), P(tp, None)),
        out_specs=P(seq, tp),
        check_vma=False,
    )
```
